32 devices in a mesh: job: 2 (over y), row: 4 (over z), col: 2 (over x), samp: 2 (over core).
Axes of the slice: x: 2, y: 2, z: 4, core: 2. Of those that a mesh axis runs over, the one named last changes fastest.
Arguments:
- pair_repr: bfloat16 [256, 128, 128], P(('job', 'row'), ('col', 'samp')), parts along dimension 0, may hold values from -100 to 100
- asym_id: int32 [256], P('job'), parts along dimension 0, may hold values from 0 to 7, never falling along the last dimension, each value on 1 to 32 neighbouring positions
- valid_len: int32 [2], P('job'), parts along dimension 0, may hold values from 64 to 128
- rel_embed: bfloat16 [128, 128], replicated, may hold values from -12 to 12
- pair_gain: float32 [128], replicated, may hold values from 0.25 to 1.75
- bias_weight: bfloat16 [128, 16], replicated, may hold values from -64 to 64
- tokens: bfloat16 [32, 128, 768], P(('job', 'col', 'samp'), 'row'), parts along dimension 0, may hold values from -6 to 6
- token_gain: float32 [1, 768], replicated, may hold values from 0.25 to 1.75
- qkv_weight: bfloat16 [1, 3, 768, 768], P(None, None, None, 'row'), may hold values from -0.21875 to 0.21875
- out_weight: bfloat16 [1, 768, 768], P(None, 'row'), may hold values from -0.21875 to 0.21875
Outputs:
- refined: bfloat16 [32, 128, 768], P(('job', 'col', 'samp'), 'row'), parts along dimension 0
The draws below stay inside these ranges and needn't reach their ends.
There are 2 independent parts, one for each index of `job`. The reference program is written for one: setup_inputs(seed, part) draws one part's arguments, and reference() takes and returns one part's arrays. A program takes and returns all parts, laid end to end along the dimension named above; an argument that names none is the same for every part. Nothing has to cross between parts.
Inputs may be any that keep to these rules, and one draw needn't show every extreme that they name: `asym_id`: chain indices never fall along the tokens.
All inputs are finite; a program needn't handle non-finite values.
Results may differ from the reference program's by a relative error of at most 0.002.
The reference program's roundings to bfloat16 on the way count: a program that leaves them out, or rounds other values in their place, can miss the bound.
Values may be sent and summed in bfloat16 or wider, within the bound.
A program may use at most 64 MiB of HBM per device.

```python
import math
import jax
import jax.numpy as jnp
import numpy as np
from jax import lax

PAIR_C = 128
D = 768
HEADS = 16
HEAD_DIM = 48
REL = 128
LAYERS = 1
TOKENS = 128
SAMPLES = 16
N_ROW = 4


def draw_pair_repr(key, part):
    noise_key, scale_key = jax.random.split(key, 2)
    scales = jnp.exp(jax.random.uniform(scale_key, (TOKENS, TOKENS, 1), jnp.float32, 0.0, math.log(10.0)))
    values = jax.random.normal(noise_key, (TOKENS, TOKENS, PAIR_C), jnp.float32) * scales
    return jnp.clip(values, -100.0, 100.0).astype(jnp.bfloat16)


def draw_bias_weight(key, part):
    noise_key = jax.random.fold_in(key, 0)
    strength = jnp.full((1, HEADS), 2.5, jnp.float32)
    spread = strength / math.sqrt(PAIR_C)
    values = jax.random.normal(noise_key, (PAIR_C, HEADS), jnp.float32) * spread
    return jnp.clip(values, -6.0 * spread, 6.0 * spread).astype(jnp.bfloat16)


def level_of(key, dims, cuts, smallest, top_value):
    factor_of, own = 1.0, jax.random.fold_in(key, 6)
    for position, shards_of in cuts:
        draws = jnp.exp(jax.random.uniform(jax.random.fold_in(own, position), (shards_of,), jnp.float32, smallest / len(cuts), top_value / len(cuts)))
        factor_of = factor_of * jnp.repeat(draws, dims[position] // shards_of).reshape([-1 if axis == position else 1 for axis in range(len(dims))])
    return factor_of


def length_profile(amount, total, most, skew):
    weights = [(1 << 20) // math.isqrt(rank ** skew) + 1 for rank in range(2, amount + 1)]
    spare, holding = total - most - (amount - 1), [1] * (amount - 1)
    while spare > 0:
        movable = [i for i in range(amount - 1) if holding[i] < most]
        pool, budget = sum([weights[i] for i in movable]), spare
        for i in movable:
            addition = min(most - holding[i], max(1, budget * weights[i] // pool), spare)
            holding[i] = holding[i] + addition
            spare = spare - addition
    return np.array([most] + holding)


def uneven(own_key, count, total, limit, skew):
    if count == 2:
        one = jax.random.randint(own_key, (), max(1, total - limit), min(limit, total - 1) + 1)
        return jnp.stack([one, total - one])
    sizes = jnp.asarray(length_profile(count, total, limit, skew), jnp.int32)
    couples = (count - 1) // 2
    giver, sink = sizes[1:1 + 2 * couples:2], sizes[2:2 + 2 * couples:2]
    room = jnp.minimum(giver - 1, limit - sink)
    moved = jax.random.randint(jax.random.fold_in(own_key, 1), (couples,), 0, 1 << 20) % (room + 1)
    sizes = sizes.at[1:1 + 2 * couples:2].set(giver - moved).at[2:2 + 2 * couples:2].set(sink + moved)
    return sizes[jax.random.permutation(jax.random.fold_in(own_key, 2), count)]


def normal_values(stream_key, shape, deviation, reach, shards=(), held_as=jnp.bfloat16):
    array = jax.random.normal(stream_key, shape, jnp.float32) * deviation
    if len(shards) > 0:
        array = level_of(stream_key, shape, shards, -0.22, 0.18) * array
    return jnp.clip(array, min=-reach, max=reach).astype(held_as)


def setup_inputs(seed: int = 0, part: int = 0) -> dict:
    arg_keys = jax.random.split(jax.random.key(seed), 11)
    own_keys = jax.random.split(jax.random.fold_in(arg_keys[10], part), 11)
    pair_repr = draw_pair_repr(jax.random.fold_in(jax.random.fold_in(arg_keys[10], part), 71), part)
    asym_id = jnp.searchsorted(jnp.cumsum(uneven(own_keys[1], 8, TOKENS, TOKENS // 4, 1)), jnp.arange(TOKENS), side="right").astype(jnp.int32)
    valid_len = jax.random.randint(own_keys[2], (1,), TOKENS // 2, TOKENS + 1).astype(jnp.int32)
    rel_embed = normal_values(arg_keys[3], (REL, PAIR_C), 2.0, 12.0)
    pair_gain = jnp.clip(1.0 + 0.15 * jax.random.normal(arg_keys[4], (PAIR_C,), jnp.float32), 0.25, 1.75)
    bias_weight = draw_bias_weight(jax.random.fold_in(arg_keys[10], 71), part)
    tokens = normal_values(own_keys[6], (SAMPLES, TOKENS, D), 1.0, 6.0, ((0, 4), (1, 4)))
    token_gain = jnp.clip(1.0 + 0.15 * jax.random.normal(arg_keys[7], (LAYERS, D), jnp.float32), 0.25, 1.75)
    qkv_weight = normal_values(arg_keys[8], (LAYERS, 3, D, D), D ** -0.5, 0.21875, ((3, 4),))
    out_weight = normal_values(arg_keys[9], (LAYERS, D, D), D ** -0.5, 0.21875, ((1, 4),))
    return dict(pair_repr=pair_repr, asym_id=asym_id, valid_len=valid_len, rel_embed=rel_embed, pair_gain=pair_gain, bias_weight=bias_weight, tokens=tokens, token_gain=token_gain, qkv_weight=qkv_weight, out_weight=out_weight)


epsilon = 1e-05

def normalize(values, gain_vector):
    average = lax.optimization_barrier(jnp.mean(values, axis=-1, keepdims=True))
    centered = values - average
    variance = lax.optimization_barrier(jnp.mean(centered * centered, axis=-1, keepdims=True))
    return centered * lax.rsqrt(variance + epsilon) * gain_vector

def attend_sample(queries, key_rows, value_rows, pair_bias, keymask):
    query_f = queries.astype(jnp.float32).reshape(TOKENS, HEADS, HEAD_DIM)
    key_f = key_rows.astype(jnp.float32).reshape(TOKENS, HEADS, HEAD_DIM)
    value_f = value_rows.astype(jnp.float32).reshape(TOKENS, HEADS, HEAD_DIM)
    scores = jnp.einsum('ihd,jhd->hij', query_f, key_f) / math.sqrt(HEAD_DIM) + pair_bias
    scores = jnp.where(keymask[None, None, :], scores, -1e+30)
    row_max = lax.optimization_barrier(jnp.max(scores, axis=-1, keepdims=True))
    weights = jnp.where(keymask[None, None, :], jnp.exp(scores - row_max), 0.0)
    row_total = lax.optimization_barrier(jnp.sum(weights, axis=-1, keepdims=True))
    probs = (weights / row_total).astype(jnp.bfloat16)
    attended = jnp.einsum('hij,jhd->ihd', probs.astype(jnp.float32), value_f)
    return attended.reshape(TOKENS, D).astype(jnp.bfloat16)

def reference(pair_repr, asym_id, valid_len, rel_embed, pair_gain, bias_weight, tokens, token_gain, qkv_weight, out_weight):
    block_rows = TOKENS // N_ROW
    positions = jnp.arange(TOKENS, dtype=jnp.int32)
    reach_max = REL // 2 - 1

    def bias_block(block_index):
        first_row = (block_index * block_rows).astype(jnp.int32)
        pair_rows = lax.dynamic_slice_in_dim(pair_repr, first_row, block_rows, 0)
        row_ids = first_row + jnp.arange(block_rows, dtype=jnp.int32)
        row_chain = lax.dynamic_slice_in_dim(asym_id, first_row, block_rows, 0)
        offset = jnp.clip(row_ids[:, None] - positions[None, :], -reach_max, reach_max) + reach_max
        bin_ids = jnp.where(row_chain[:, None] == asym_id[None, :], offset, REL - 1)
        onehot = (bin_ids.reshape(-1)[:, None] == jnp.arange(REL, dtype=jnp.int32)[None, :]).astype(jnp.bfloat16)
        summed = pair_rows.reshape(-1, PAIR_C).astype(jnp.float32) + jnp.dot(onehot, rel_embed, preferred_element_type=jnp.float32)
        normed = normalize(summed, pair_gain).astype(jnp.bfloat16)
        projected = lax.dot_general(bias_weight, normed, (((0,), (1,)), ((), ())), preferred_element_type=jnp.float32)
        return projected.reshape(HEADS, block_rows, TOKENS)
    blocks = lax.map(bias_block, jnp.arange(N_ROW, dtype=jnp.int32))
    pair_bias = jnp.transpose(blocks, (1, 0, 2, 3)).reshape(HEADS, TOKENS, TOKENS)
    keymask = positions < valid_len[0]
    current = tokens
    for layer_index in range(LAYERS):
        normed_tok = normalize(current.astype(jnp.float32), token_gain[layer_index]).astype(jnp.bfloat16)
        flat = normed_tok.reshape(-1, D)
        parts = []
        for part_index in range(3):
            product = jnp.dot(flat, qkv_weight[layer_index, part_index], preferred_element_type=jnp.float32)
            parts.append(product.astype(jnp.bfloat16).reshape(SAMPLES, TOKENS, D))

        def one_sample(sample_item):
            return attend_sample(sample_item[0], sample_item[1], sample_item[2], pair_bias, keymask)
        attended = lax.map(one_sample, (parts[0], parts[1], parts[2]))
        update = jnp.dot(attended.reshape(-1, D), out_weight[layer_index], preferred_element_type=jnp.float32)
        current = (current.astype(jnp.float32) + update.reshape(SAMPLES, TOKENS, D)).astype(jnp.bfloat16)
    return current
```

```python
import functools
import math

import jax
import jax.numpy as jnp
from jax import lax
from jax.experimental import pallas as pl
from jax.experimental.pallas import tpu as pltpu
from jax.sharding import PartitionSpec as P

HEAD_DIM = 48
EPSILON = 1e-05
LANES = 128
MESH = pl.DeviceIdType.MESH


def normalize(values, gain_vector):
    average = jnp.mean(values, axis=-1, keepdims=True)
    centered = values - average
    variance = jnp.mean(centered * centered, axis=-1, keepdims=True)
    return centered * lax.rsqrt(variance + EPSILON) * gain_vector


def kernel(
    axes,
    asym,
    valid,
    pair_hbm,
    rel_hbm,
    pair_gain_hbm,
    bias_weight_hbm,
    tokens_hbm,
    token_gain_hbm,
    qkv_hbm,
    out_weight_hbm,
    out,
    pair,
    rel,
    pair_gain,
    bias_weight,
    token_gain,
    qkv,
    tok,
    ow,
    bias_send,
    bias_recv,
    bias,
    query,
    key,
    value,
    attended,
    heads_in,
    local_sem,
    tok_local,
    tok_send,
    tok_recv,
    bz_send,
    bz_recv,
    bp_send,
    bp_recv,
    own_bias_sem,
    oz_send,
    oz_recv,
    op_send,
    op_recv,
    at_send,
    at_recv,
):
    n_job, n_row, n_col, n_samp = axes
    job, me = lax.axis_index("job"), lax.axis_index("row")
    col, samp = lax.axis_index("col"), lax.axis_index("samp")
    samples, token_rows, width = tokens_hbm.shape
    total = n_row * token_rows
    tile_rows, tile_cols, channels = pair.shape
    bins = rel.shape[0]
    n_plane = n_col * n_samp
    plane = col * n_samp + samp
    all_heads = bias_weight.shape[1]
    local_heads = all_heads // n_row
    head_rows = bias_recv.shape[2]
    fold = LANES // tile_cols
    stripes = tile_rows // fold
    out_rows = ow.shape[1]
    pieces = oz_recv.shape[0] // n_row
    piece_rows = out_rows // pieces
    shared = pieces > 1
    group = job * n_samp + samp if shared else 0
    local_width = local_heads * HEAD_DIM

    def row_peer(k):
        return lax.rem(me + k, n_row)

    def plane_peer(k):
        other = lax.rem(plane + k, n_plane)
        return {"col": lax.div(other, n_samp), "samp": lax.rem(other, n_samp)}, other

    def group_peer(k):
        other = lax.rem(group + k, pieces)
        return {"job": lax.div(other, n_samp), "samp": lax.rem(other, n_samp)}, other

    loads = {}
    for index, (name, source, target) in enumerate(
        (
            ("pair", pair_hbm, pair),
            ("rel", rel_hbm, rel),
            ("pair_gain", pair_gain_hbm, pair_gain),
            ("bias_weight", bias_weight_hbm, bias_weight),
            ("token_gain", token_gain_hbm, token_gain),
            ("qkv", qkv_hbm.at[0], qkv),
            ("ow", out_weight_hbm.at[0], ow.at[me]),
        )
    ):
        loads[name] = pltpu.make_async_copy(source, target, local_sem.at[index])
    tok_loads = [
        pltpu.make_async_copy(tokens_hbm.at[s], tok.at[s, me], tok_local.at[s]) for s in range(samples)
    ]
    tok_loads[0].start()
    for name in ("pair", "rel", "pair_gain", "bias_weight"):
        loads[name].start()
    for s in range(1, samples):
        tok_loads[s].start()
    for name in ("token_gain", "qkv", "ow"):
        loads[name].start()

    barrier = pltpu.get_barrier_semaphore()
    for k in range(1, n_row):
        pl.semaphore_signal(barrier, inc=1, device_id={"row": row_peer(k)}, device_id_type=MESH)
    for k in range(1, n_plane):
        pl.semaphore_signal(barrier, inc=1, device_id=plane_peer(k)[0], device_id_type=MESH)
    if shared:
        for k in range(1, pieces):
            pl.semaphore_signal(barrier, inc=1, device_id=group_peer(k)[0], device_id_type=MESH)
    pl.semaphore_wait(barrier, (n_row - 1) + (n_plane - 1) + ((pieces - 1) if shared else 0))

    has_right, has_left = me < n_row - 1, me > 0
    right, left = jnp.minimum(me + 1, n_row - 1), jnp.maximum(me - 1, 0)

    def tok_copy(s, source, direction):
        return pltpu.make_async_remote_copy(
            src_ref=tok.at[s, source],
            dst_ref=tok.at[s, source],
            send_sem=tok_send.at[direction, s, source],
            recv_sem=tok_recv.at[s, source],
            device_id={"row": left if direction else right},
            device_id_type=MESH,
        )

    def send_own(s):
        tok_loads[s].wait()

        @pl.when(has_right)
        def _():
            tok_copy(s, me, 0).start()

        @pl.when(has_left)
        def _():
            tok_copy(s, me, 1).start()

    def pass_on(s):
        for k in range(1, n_row):

            @pl.when(me - k >= 0)
            def _():
                source = jnp.maximum(me - k, 0)
                tok_copy(s, source, 0).wait_recv()

                @pl.when(has_right)
                def _():
                    tok_copy(s, source, 0).start()

            @pl.when(me + k < n_row)
            def _():
                source = jnp.minimum(me + k, n_row - 1)
                tok_copy(s, source, 1).wait_recv()

                @pl.when(has_left)
                def _():
                    tok_copy(s, source, 1).start()

    def finish_tok_sends(s):
        for k in range(0, n_row):

            @pl.when(jnp.logical_and(me - k >= 0, has_right))
            def _():
                tok_copy(s, jnp.maximum(me - k, 0), 0).wait_send()

            @pl.when(jnp.logical_and(me + k < n_row, has_left))
            def _():
                tok_copy(s, jnp.minimum(me + k, n_row - 1), 1).wait_send()

    for s in range(min(2, samples)):
        send_own(s)

    for name in ("pair", "rel", "pair_gain", "bias_weight"):
        loads[name].wait()
    first_row, first_col = me * tile_rows, plane * tile_cols
    sub = lax.broadcasted_iota(jnp.int32, (tile_cols, LANES), 0)
    lane = lax.broadcasted_iota(jnp.int32, (tile_cols, LANES), 1)
    col_chain = jnp.zeros((tile_cols, LANES), jnp.int32)
    for j in range(tile_cols):
        col_chain = jnp.where(sub == j, asym[first_col + j], col_chain)
    reach = bins // 2 - 1
    turned_weight = bias_weight[...].astype(jnp.float32).T.astype(jnp.bfloat16)
    for t in range(stripes):
        hots, rows = [], []
        for q in range(fold):
            i = q * stripes + t
            offset = jnp.clip(first_row + i - first_col - sub, -reach, reach) + reach
            bin_ids = jnp.where(col_chain == asym[first_row + i], offset, bins - 1)
            hots.append(jnp.where(bin_ids == lane, 1.0, 0.0).astype(jnp.bfloat16))
            rows.append(pair[i].astype(jnp.float32))
        summed = jnp.concatenate(rows, axis=0) + jnp.dot(
            jnp.concatenate(hots, axis=0), rel[...], preferred_element_type=jnp.float32
        )
        normed = normalize(summed, pair_gain[...]).astype(jnp.bfloat16)
        projected = lax.dot_general(
            turned_weight, normed, (((1,), (1,)), ((), ())), preferred_element_type=jnp.float32
        )
        bias_send[pl.ds(t, all_heads, stride=stripes), :] = projected

    def bias_part(dest):
        return bias_send.at[pl.ds(pl.multiple_of(dest * head_rows, head_rows), head_rows)]

    def bias_row_copy(k):
        dest = row_peer(k)
        return pltpu.make_async_remote_copy(
            src_ref=bias_part(dest),
            dst_ref=bias_recv.at[me, plane],
            send_sem=bz_send.at[k],
            recv_sem=bz_recv.at[k],
            device_id={"row": dest},
            device_id_type=MESH,
        )

    def bias_plane_copy(k, m):
        device, _ = plane_peer(m)
        source = row_peer(n_row - k)
        return pltpu.make_async_remote_copy(
            src_ref=bias_part(me) if k == 0 else bias_recv.at[source, plane],
            dst_ref=bias_recv.at[source, plane],
            send_sem=bp_send.at[k, m],
            recv_sem=bp_recv.at[k, m],
            device_id=device,
            device_id_type=MESH,
        )

    def bias_plane_wait(k, m):
        source = row_peer(n_row - k)
        origin = lax.rem(plane + n_plane - m, n_plane)
        pltpu.make_async_remote_copy(
            src_ref=bias_recv.at[source, origin],
            dst_ref=bias_recv.at[source, origin],
            send_sem=bp_send.at[k, m],
            recv_sem=bp_recv.at[k, m],
            device_id=plane_peer(m)[0],
            device_id_type=MESH,
        ).wait_recv()

    def bias_row_wait(k):
        source = row_peer(n_row - k)
        pltpu.make_async_remote_copy(
            src_ref=bias_recv.at[source, plane],
            dst_ref=bias_recv.at[source, plane],
            send_sem=bz_send.at[k],
            recv_sem=bz_recv.at[k],
            device_id={"row": row_peer(k)},
            device_id_type=MESH,
        ).wait_recv()

    for k in range(1, n_row):
        bias_row_copy(k).start()
    own_bias = pltpu.make_async_copy(bias_part(me), bias_recv.at[me, plane], own_bias_sem)
    own_bias.start()
    for m in range(1, n_plane):
        bias_plane_copy(0, m).start()

    def ow_part(source, piece):
        if not shared:
            return ow.at[source]
        return ow.at[source, pl.ds(pl.multiple_of(piece * piece_rows, piece_rows), piece_rows)]

    def ow_row_copy(k):
        return pltpu.make_async_remote_copy(
            src_ref=ow_part(me, group),
            dst_ref=ow_part(me, group),
            send_sem=oz_send.at[k],
            recv_sem=oz_recv.at[k],
            device_id={"row": row_peer(k)},
            device_id_type=MESH,
        )

    def ow_row_wait(k):
        source = row_peer(n_row - k)
        pltpu.make_async_remote_copy(
            src_ref=ow_part(source, group),
            dst_ref=ow_part(source, group),
            send_sem=oz_send.at[k],
            recv_sem=oz_recv.at[k],
            device_id={"row": row_peer(k)},
            device_id_type=MESH,
        ).wait_recv()

    def ow_group_copy(k, m):
        source = row_peer(n_row - k)
        return pltpu.make_async_remote_copy(
            src_ref=ow_part(source, group),
            dst_ref=ow_part(source, group),
            send_sem=op_send.at[k, m],
            recv_sem=op_recv.at[k, m],
            device_id=group_peer(m)[0],
            device_id_type=MESH,
        )

    def ow_group_wait(k, m):
        source = row_peer(n_row - k)
        origin = lax.rem(group + pieces - m, pieces)
        pltpu.make_async_remote_copy(
            src_ref=ow_part(source, origin),
            dst_ref=ow_part(source, origin),
            send_sem=op_send.at[k, m],
            recv_sem=op_recv.at[k, m],
            device_id=group_peer(m)[0],
            device_id_type=MESH,
        ).wait_recv()

    head_of_lane = lax.broadcasted_iota(jnp.int32, (total, local_width), 1)
    head_masks = [
        jnp.logical_and(head_of_lane >= h * HEAD_DIM, head_of_lane < (h + 1) * HEAD_DIM)
        for h in range(local_heads)
    ]
    scale = 1.0 / math.sqrt(HEAD_DIM)

    def project(s):
        rows = tok[s].reshape(total, width).astype(jnp.float32)
        normed = normalize(rows, token_gain[...]).astype(jnp.bfloat16)
        query[s] = jnp.dot(normed, qkv[0], preferred_element_type=jnp.float32).astype(jnp.bfloat16)
        key[s] = jnp.dot(normed, qkv[1], preferred_element_type=jnp.float32).astype(jnp.bfloat16)
        value[s] = jnp.dot(normed, qkv[2], preferred_element_type=jnp.float32).astype(jnp.bfloat16)

    def attend(s):
        keys, values = key[s].astype(jnp.float32), value[s].astype(jnp.float32)
        keys = jnp.concatenate(
            [jnp.where(mask, keys, 0.0).astype(jnp.bfloat16) for mask in head_masks], axis=0
        )
        values = jnp.concatenate(
            [jnp.where(mask, values, 0.0).astype(jnp.bfloat16) for mask in head_masks], axis=0
        )
        scores = lax.dot_general(
            query[s], keys, (((1,), (1,)), ((), ())), preferred_element_type=jnp.float32
        )
        probs = []
        for h in range(local_heads):
            mine = scores[:, h * total : (h + 1) * total] * scale + bias[:, h * total : (h + 1) * total]
            weights = jnp.exp(mine - jnp.max(mine, axis=-1, keepdims=True))
            inverse = 1.0 / jnp.sum(weights, axis=-1, keepdims=True)
            probs.append((weights * inverse).astype(jnp.bfloat16))
        mixed = jnp.dot(
            jnp.concatenate(probs, axis=1), values, preferred_element_type=jnp.float32
        ).astype(jnp.bfloat16)
        attended[s] = mixed.reshape(n_row, token_rows, local_width)

    def att_copy(s, k):
        dest = row_peer(k)
        return pltpu.make_async_remote_copy(
            src_ref=attended.at[s, dest],
            dst_ref=heads_in.at[me, s],
            send_sem=at_send.at[s, k],
            recv_sem=at_recv.at[s, k],
            device_id={"row": dest},
            device_id_type=MESH,
        )

    def att_wait(s, k):
        source = row_peer(n_row - k)
        pltpu.make_async_remote_copy(
            src_ref=heads_in.at[source, s],
            dst_ref=heads_in.at[source, s],
            send_sem=at_send.at[s, k],
            recv_sem=at_recv.at[s, k],
            device_id={"row": row_peer(k)},
            device_id_type=MESH,
        ).wait_recv()

    def give(s):
        for k in range(1, n_row):
            att_copy(s, k).start()
        heads_in[me, s] = attended[s, me]

    pass_on(0)
    for s in range(2, min(3, samples)):
        send_own(s)
    for k in range(1, n_row):
        bias_row_wait(k)
        for m in range(1, n_plane):
            bias_plane_copy(k, m).start()
    for name in ("token_gain", "qkv"):
        loads[name].wait()
    project(0)
    for s in range(1, samples):
        pass_on(s)
        if s + 2 < samples:
            send_own(s + 2)
        if s == 1:
            loads["ow"].wait()
            for k in range(1, n_row):
                ow_row_copy(k).start()
        project(s)
        if s == 1:
            own_bias.wait()
            for k in range(n_row):
                for m in range(1, n_plane):
                    bias_plane_wait(k, m)
            lanes_at = lax.broadcasted_iota(jnp.int32, (head_rows, LANES), 1)
            for tile in range(total // LANES):
                padded = lanes_at[:stripes] + tile * LANES >= valid[0]
                for r in range(n_row):
                    parts = [bias_recv[r, tile * fold + m] for m in range(fold)]
                    for q in range(fold):
                        whole = None
                        for m in range(fold):
                            shift = ((m - q) % fold) * tile_cols
                            turned = pltpu.roll(parts[m], shift, 1) if shift else parts[m]
                            whole = (
                                turned
                                if whole is None
                                else jnp.where(lanes_at >= m * tile_cols, turned, whole)
                            )
                        at = r * tile_rows + q * stripes
                        for h in range(local_heads):
                            bias[
                                at : at + stripes,
                                h * total + tile * LANES : h * total + (tile + 1) * LANES,
                            ] = jnp.where(padded, -1e30, whole[h * stripes : (h + 1) * stripes])
        if s == 2 and shared:
            for k in range(1, n_row):
                ow_row_wait(k)
                for m in range(1, pieces):
                    ow_group_copy(k, m).start()
        attend(s - 1)
        give(s - 1)
    attend(samples - 1)
    give(samples - 1)

    for k in range(1, n_row):
        if shared:
            for m in range(1, pieces):
                ow_group_wait(k, m)
        else:
            ow_row_wait(k)

    def update_of(source):
        flat = heads_in[source].reshape(samples * token_rows, local_width)
        return jnp.dot(flat, ow[source], preferred_element_type=jnp.float32)

    update = tok[:, me].reshape(samples * token_rows, width).astype(jnp.float32) + 0.0
    product = update_of(me)
    for k in range(1, n_row):
        for s in range(samples):
            att_wait(s, k)
        product = product + update_of(row_peer(n_row - k))
    out[...] = (update + product).astype(out.dtype).reshape(samples, token_rows, width)

    for s in range(samples):
        finish_tok_sends(s)
        for k in range(1, n_row):
            att_copy(s, k).wait_send()
    for k in range(1, n_row):
        bias_row_copy(k).wait_send()
        ow_row_copy(k).wait_send()
        if shared:
            for m in range(1, pieces):
                ow_group_copy(k, m).wait_send()
    for k in range(n_row):
        for m in range(1, n_plane):
            bias_plane_copy(k, m).wait_send()


def per_device(
    axes,
    pair_repr,
    asym_id,
    valid_len,
    rel_embed,
    pair_gain,
    bias_weight,
    tokens,
    token_gain,
    qkv_weight,
    out_weight,
):
    n_job, n_row, n_col, n_samp = axes
    samples, token_rows, width = tokens.shape
    total = n_row * token_rows
    n_plane = n_col * n_samp
    heads = bias_weight.shape[1]
    local_heads = heads // n_row
    tile_rows, tile_cols, channels = pair_repr.shape
    local_width = qkv_weight.shape[-1]
    out_rows = out_weight.shape[1]
    pieces = n_job * n_samp
    if out_rows % (16 * pieces) or pieces == 1:
        pieces = 1
    stripes = tile_rows // (LANES // tile_cols)
    head_rows = local_heads * stripes
    bf16, f32 = jnp.bfloat16, jnp.float32
    dma = pltpu.SemaphoreType.DMA
    any_spec = pl.BlockSpec(memory_space=pl.ANY)
    smem_spec = pl.BlockSpec(memory_space=pltpu.SMEM)
    return pl.pallas_call(
        functools.partial(kernel, axes),
        out_shape=jax.ShapeDtypeStruct(tokens.shape, tokens.dtype),
        in_specs=[smem_spec] * 2 + [any_spec] * 8,
        out_specs=pl.BlockSpec(memory_space=pltpu.VMEM),
        scratch_shapes=[
            pltpu.VMEM(pair_repr.shape, bf16),
            pltpu.VMEM(rel_embed.shape, bf16),
            pltpu.VMEM((1, channels), f32),
            pltpu.VMEM(bias_weight.shape, bf16),
            pltpu.VMEM(token_gain.shape, f32),
            pltpu.VMEM(qkv_weight.shape[1:], bf16),
            pltpu.VMEM((samples, n_row, token_rows, width), bf16),
            pltpu.VMEM((n_row, out_rows, width), bf16),
            pltpu.VMEM((heads * stripes, LANES), f32),
            pltpu.VMEM((n_row, n_plane, head_rows, LANES), f32),
            pltpu.VMEM((total, local_heads * total), f32),
            pltpu.VMEM((samples, total, local_width), bf16),
            pltpu.VMEM((samples, total, local_width), bf16),
            pltpu.VMEM((samples, total, local_width), bf16),
            pltpu.VMEM((samples, n_row, token_rows, local_width), bf16),
            pltpu.VMEM((n_row, samples, token_rows, local_width), bf16),
            dma((7,)),
            dma((samples,)),
            dma((2, samples, n_row)),
            dma((samples, n_row)),
            dma((n_row,)),
            dma((n_row,)),
            dma((n_row, n_plane)),
            dma((n_row, n_plane)),
            dma,
            dma((n_row,)),
            dma((n_row * pieces,)),
            dma((n_row, pieces)),
            dma((n_row, pieces)),
            dma((samples, n_row)),
            dma((samples, n_row)),
        ],
        compiler_params=pltpu.CompilerParams(
            collective_id=0, has_side_effects=True, vmem_limit_bytes=60 * 1024 * 1024
        ),
    )(
        asym_id,
        valid_len,
        pair_repr,
        rel_embed,
        pair_gain.reshape(1, channels),
        bias_weight,
        tokens,
        token_gain,
        qkv_weight,
        out_weight,
    )


def solution(mesh):
    axes = tuple(mesh.shape[name] for name in ("job", "row", "col", "samp"))
    return jax.shard_map(
        functools.partial(per_device, axes),
        mesh=mesh,
        in_specs=(
            P(("job", "row"), ("col", "samp"), None),
            P("job"),
            P("job"),
            P(),
            P(),
            P(),
            P(("job", "col", "samp"), "row", None),
            P(),
            P(None, None, None, "row"),
            P(None, "row", None),
        ),
        out_specs=P(("job", "col", "samp"), "row", None),
        check_vma=False,
    )
```

```python
import functools
import math

import jax
import jax.numpy as jnp
from jax import lax
from jax.experimental import pallas as pl
from jax.experimental.pallas import tpu as pltpu
from jax.sharding import PartitionSpec as P

HEAD_DIM = 48
EPSILON = 1e-05
LANES = 128
MESH = pl.DeviceIdType.MESH


def normalize(values, gain_vector):
    average = jnp.mean(values, axis=-1, keepdims=True)
    centered = values - average
    variance = jnp.mean(centered * centered, axis=-1, keepdims=True)
    return centered * lax.rsqrt(variance + EPSILON) * gain_vector


def kernel(
    axes,
    split,
    asym_hbm,
    valid_hbm,
    pair_hbm,
    rel_hbm,
    pair_gain_hbm,
    bias_weight_hbm,
    tokens_hbm,
    token_gain_hbm,
    qkv_hbm,
    out_weight_hbm,
    out,
    asym,
    valid,
    pair,
    rel,
    pair_gain,
    bias_weight,
    token_gain,
    qkv,
    tok,
    ow,
    bias_send,
    bias_recv,
    bias,
    query,
    key,
    value,
    attended,
    heads_in,
    local_sem,
    tok_local,
    tok_send,
    tok_recv,
    bz_send,
    bz_recv,
    bp_send,
    bp_recv,
    own_bias_sem,
    oz_send,
    oz_recv,
    op_send,
    op_recv,
    at_send,
    at_recv,
):
    n_job, n_row, n_col, n_samp = axes
    job, me = lax.axis_index("job"), lax.axis_index("row")
    col, samp = lax.axis_index("col"), lax.axis_index("samp")
    samples, token_rows, width = tokens_hbm.shape
    total = n_row * token_rows
    tile_rows, tile_cols, channels = pair.shape
    bins = rel.shape[0]
    n_plane = n_col * n_samp
    plane = col * n_samp + samp
    all_heads = bias_weight.shape[0]
    local_heads = all_heads // n_row
    head_rows = bias_recv.shape[2]
    fold = LANES // tile_cols
    stripes = tile_rows // fold
    out_rows = ow.shape[1]
    row_pieces, col_pieces = split
    pieces = row_pieces * col_pieces
    piece_rows, piece_cols = out_rows // row_pieces, width // col_pieces
    shared = pieces > 1
    group = (job * n_samp + samp if row_pieces > 1 else 0) * col_pieces + (
        col if col_pieces > 1 else 0
    )
    local_width = local_heads * HEAD_DIM

    def row_peer(k):
        return lax.rem(me + k, n_row)

    def plane_peer(k):
        other = lax.rem(plane + k, n_plane)
        return {"col": lax.div(other, n_samp), "samp": lax.rem(other, n_samp)}, other

    def group_peer(k):
        other = lax.rem(group + k, pieces)
        device, held = {}, lax.div(other, col_pieces)
        if row_pieces > 1:
            device.update(job=lax.div(held, n_samp), samp=lax.rem(held, n_samp))
        if col_pieces > 1:
            device.update(col=lax.rem(other, col_pieces))
        return device, other

    loads = {}
    for index, (name, source, target) in enumerate(
        (
            ("asym", asym_hbm, asym),
            ("valid", valid_hbm, valid),
            ("pair", pair_hbm, pair),
            ("rel", rel_hbm, rel),
            ("pair_gain", pair_gain_hbm, pair_gain),
            ("bias_weight", bias_weight_hbm, bias_weight),
            ("token_gain", token_gain_hbm, token_gain),
            ("qkv", qkv_hbm.at[0], qkv),
            ("ow", out_weight_hbm.at[0], ow.at[me]),
        )
    ):
        loads[name] = pltpu.make_async_copy(source, target, local_sem.at[index])
    tok_loads = [
        pltpu.make_async_copy(tokens_hbm.at[s], tok.at[s, me], tok_local.at[s]) for s in range(samples)
    ]
    tok_loads[0].start()
    for name in ("asym", "pair", "rel", "pair_gain", "bias_weight", "valid"):
        loads[name].start()
    for s in range(1, samples):
        tok_loads[s].start()
    for name in ("token_gain", "qkv", "ow"):
        loads[name].start()

    barrier = pltpu.get_barrier_semaphore()
    for k in range(1, n_row):
        pl.semaphore_signal(barrier, inc=1, device_id={"row": row_peer(k)}, device_id_type=MESH)
    for k in range(1, n_plane):
        pl.semaphore_signal(barrier, inc=1, device_id=plane_peer(k)[0], device_id_type=MESH)
    if shared:
        for k in range(1, pieces):
            pl.semaphore_signal(barrier, inc=1, device_id=group_peer(k)[0], device_id_type=MESH)
    pl.semaphore_wait(barrier, (n_row - 1) + (n_plane - 1) + ((pieces - 1) if shared else 0))

    has_right, has_left = me < n_row - 1, me > 0
    right, left = jnp.minimum(me + 1, n_row - 1), jnp.maximum(me - 1, 0)

    def tok_copy(s, source, direction):
        return pltpu.make_async_remote_copy(
            src_ref=tok.at[s, source],
            dst_ref=tok.at[s, source],
            send_sem=tok_send.at[direction, s, source],
            recv_sem=tok_recv.at[s, source],
            device_id={"row": left if direction else right},
            device_id_type=MESH,
        )

    def send_own(s):
        tok_loads[s].wait()

        @pl.when(has_right)
        def _():
            tok_copy(s, me, 0).start()

        @pl.when(has_left)
        def _():
            tok_copy(s, me, 1).start()

    def pass_on(k, s):
        @pl.when(me - k >= 0)
        def _():
            source = jnp.maximum(me - k, 0)
            tok_copy(s, source, 0).wait_recv()

            @pl.when(has_right)
            def _():
                tok_copy(s, source, 0).start()

        @pl.when(me + k < n_row)
        def _():
            source = jnp.minimum(me + k, n_row - 1)
            tok_copy(s, source, 1).wait_recv()

            @pl.when(has_left)
            def _():
                tok_copy(s, source, 1).start()

    def finish_tok_sends(s):
        for k in range(0, n_row):

            @pl.when(jnp.logical_and(me - k >= 0, has_right))
            def _():
                tok_copy(s, jnp.maximum(me - k, 0), 0).wait_send()

            @pl.when(jnp.logical_and(me + k < n_row, has_left))
            def _():
                tok_copy(s, jnp.minimum(me + k, n_row - 1), 1).wait_send()

    for s in range(samples):
        send_own(s)

    for name in ("asym", "pair", "rel", "pair_gain", "bias_weight", "valid"):
        loads[name].wait()
    first_row, first_col = me * tile_rows, plane * tile_cols
    sub = lax.broadcasted_iota(jnp.int32, (tile_cols, LANES), 0)
    lane = lax.broadcasted_iota(jnp.int32, (tile_cols, LANES), 1)
    col_chain = jnp.zeros((tile_cols, LANES), jnp.int32)
    for j in range(tile_cols):
        col_chain = jnp.where(sub == j, asym[first_col + j], col_chain)
    reach = bins // 2 - 1
    turned_weight = bias_weight[...]
    for t in range(stripes):
        hots, rows = [], []
        for q in range(fold):
            i = q * stripes + t
            offset = jnp.clip(first_row + i - first_col - sub, -reach, reach) + reach
            bin_ids = jnp.where(col_chain == asym[first_row + i], offset, bins - 1)
            hots.append(jnp.where(bin_ids == lane, 1.0, 0.0).astype(jnp.bfloat16))
            rows.append(pair[i].astype(jnp.float32))
        summed = jnp.concatenate(rows, axis=0) + jnp.dot(
            jnp.concatenate(hots, axis=0), rel[...], preferred_element_type=jnp.float32
        )
        normed = normalize(summed, pair_gain[...]).astype(jnp.bfloat16)
        projected = lax.dot_general(
            turned_weight, normed, (((1,), (1,)), ((), ())), preferred_element_type=jnp.float32
        )
        bias_send[pl.ds(t, all_heads, stride=stripes), :] = projected

    def bias_part(dest):
        return bias_send.at[pl.ds(pl.multiple_of(dest * head_rows, head_rows), head_rows)]

    def bias_row_copy(k):
        dest = row_peer(k)
        return pltpu.make_async_remote_copy(
            src_ref=bias_part(dest),
            dst_ref=bias_recv.at[me, plane],
            send_sem=bz_send.at[k],
            recv_sem=bz_recv.at[k],
            device_id={"row": dest},
            device_id_type=MESH,
        )

    def bias_plane_copy(k, m):
        device, _ = plane_peer(m)
        source = row_peer(n_row - k)
        return pltpu.make_async_remote_copy(
            src_ref=bias_part(me) if k == 0 else bias_recv.at[source, plane],
            dst_ref=bias_recv.at[source, plane],
            send_sem=bp_send.at[k, m],
            recv_sem=bp_recv.at[k, m],
            device_id=device,
            device_id_type=MESH,
        )

    def bias_plane_wait(k, m):
        source = row_peer(n_row - k)
        origin = lax.rem(plane + n_plane - m, n_plane)
        pltpu.make_async_remote_copy(
            src_ref=bias_recv.at[source, origin],
            dst_ref=bias_recv.at[source, origin],
            send_sem=bp_send.at[k, m],
            recv_sem=bp_recv.at[k, m],
            device_id=plane_peer(m)[0],
            device_id_type=MESH,
        ).wait_recv()

    def bias_row_wait(k):
        source = row_peer(n_row - k)
        pltpu.make_async_remote_copy(
            src_ref=bias_recv.at[source, plane],
            dst_ref=bias_recv.at[source, plane],
            send_sem=bz_send.at[k],
            recv_sem=bz_recv.at[k],
            device_id={"row": row_peer(k)},
            device_id_type=MESH,
        ).wait_recv()

    for k in range(1, n_row):
        bias_row_copy(k).start()
    own_bias = pltpu.make_async_copy(bias_part(me), bias_recv.at[me, plane], own_bias_sem)
    own_bias.start()
    for m in range(1, n_plane):
        bias_plane_copy(0, m).start()

    def ow_part(source, piece):
        if not shared:
            return ow.at[source]
        first = pl.multiple_of(lax.div(piece, col_pieces) * piece_rows, piece_rows)
        start = pl.multiple_of(lax.rem(piece, col_pieces) * piece_cols, piece_cols)
        return ow.at[source, pl.ds(first, piece_rows), pl.ds(start, piece_cols)]

    def ow_row_copy(k):
        return pltpu.make_async_remote_copy(
            src_ref=ow_part(me, group),
            dst_ref=ow_part(me, group),
            send_sem=oz_send.at[k],
            recv_sem=oz_recv.at[k],
            device_id={"row": row_peer(k)},
            device_id_type=MESH,
        )

    def ow_row_wait(k):
        source = row_peer(n_row - k)
        pltpu.make_async_remote_copy(
            src_ref=ow_part(source, group),
            dst_ref=ow_part(source, group),
            send_sem=oz_send.at[k],
            recv_sem=oz_recv.at[k],
            device_id={"row": row_peer(k)},
            device_id_type=MESH,
        ).wait_recv()

    def ow_group_copy(k, m):
        source = row_peer(n_row - k)
        return pltpu.make_async_remote_copy(
            src_ref=ow_part(source, group),
            dst_ref=ow_part(source, group),
            send_sem=op_send.at[k, m],
            recv_sem=op_recv.at[k, m],
            device_id=group_peer(m)[0],
            device_id_type=MESH,
        )

    def ow_group_wait(k, m):
        source = row_peer(n_row - k)
        origin = lax.rem(group + pieces - m, pieces)
        pltpu.make_async_remote_copy(
            src_ref=ow_part(source, origin),
            dst_ref=ow_part(source, origin),
            send_sem=op_send.at[k, m],
            recv_sem=op_recv.at[k, m],
            device_id=group_peer(m)[0],
            device_id_type=MESH,
        ).wait_recv()

    head_of_lane = lax.broadcasted_iota(jnp.int32, (total, local_width), 1)
    head_masks = [
        jnp.logical_and(head_of_lane >= h * HEAD_DIM, head_of_lane < (h + 1) * HEAD_DIM)
        for h in range(local_heads)
    ]
    scale = 1.0 / math.sqrt(HEAD_DIM)

    def project(s):
        rows = tok[s].reshape(total, width).astype(jnp.float32)
        normed = normalize(rows, token_gain[...]).astype(jnp.bfloat16)
        for index, target in enumerate((query, key, value)):
            target[s] = lax.dot_general(
                normed, qkv[index], (((1,), (1,)), ((), ())), preferred_element_type=jnp.float32
            ).astype(jnp.bfloat16)

    def attend(s):
        keys, values = key[s].astype(jnp.float32), value[s].astype(jnp.float32)
        keys = jnp.concatenate(
            [jnp.where(mask, keys, 0.0).astype(jnp.bfloat16) for mask in head_masks], axis=0
        )
        values = jnp.concatenate(
            [jnp.where(mask, values, 0.0).astype(jnp.bfloat16) for mask in head_masks], axis=0
        )
        scores = lax.dot_general(
            query[s], keys, (((1,), (1,)), ((), ())), preferred_element_type=jnp.float32
        )
        probs = []
        for h in range(local_heads):
            mine = scores[:, h * total : (h + 1) * total] * scale + bias[:, h * total : (h + 1) * total]
            weights = jnp.exp(mine - jnp.max(mine, axis=-1, keepdims=True))
            inverse = 1.0 / jnp.sum(weights, axis=-1, keepdims=True)
            probs.append((weights * inverse).astype(jnp.bfloat16))
        mixed = jnp.dot(
            jnp.concatenate(probs, axis=1), values, preferred_element_type=jnp.float32
        ).astype(jnp.bfloat16)
        attended[s] = mixed.reshape(n_row, token_rows, local_width)

    def att_copy(s, k):
        dest = row_peer(k)
        return pltpu.make_async_remote_copy(
            src_ref=attended.at[s, dest],
            dst_ref=heads_in.at[me, s],
            send_sem=at_send.at[s, k],
            recv_sem=at_recv.at[s, k],
            device_id={"row": dest},
            device_id_type=MESH,
        )

    def att_wait(s, k):
        source = row_peer(n_row - k)
        pltpu.make_async_remote_copy(
            src_ref=heads_in.at[source, s],
            dst_ref=heads_in.at[source, s],
            send_sem=at_send.at[s, k],
            recv_sem=at_recv.at[s, k],
            device_id={"row": row_peer(k)},
            device_id_type=MESH,
        ).wait_recv()

    def give(s):
        for k in range(1, n_row):
            att_copy(s, k).start()
        heads_in[me, s] = attended[s, me]

    loads["ow"].wait()
    for k in range(1, n_row):
        ow_row_copy(k).start()
    for s in range(samples):
        pass_on(1, s)
    for k in range(1, n_row):
        bias_row_wait(k)
        for m in range(1, n_plane):
            bias_plane_copy(k, m).start()
    if shared:
        for k in range(1, n_row):
            ow_row_wait(k)
            for m in range(1, pieces):
                ow_group_copy(k, m).start()
    for k in range(2, n_row - 1):
        for s in range(samples):
            pass_on(k, s)
    for name in ("token_gain", "qkv"):
        loads[name].wait()

    own_bias.wait()
    for k in range(n_row):
        for m in range(1, n_plane):
            bias_plane_wait(k, m)
    lanes_at = lax.broadcasted_iota(jnp.int32, (head_rows, LANES), 1)
    for tile in range(total // LANES):
        padded = lanes_at[:stripes] + tile * LANES >= valid[0]
        for r in range(n_row):
            parts = [bias_recv[r, tile * fold + m] for m in range(fold)]
            for q in range(fold):
                whole = None
                for m in range(fold):
                    shift = ((m - q) % fold) * tile_cols
                    turned = pltpu.roll(parts[m], shift, 1) if shift else parts[m]
                    whole = (
                        turned
                        if whole is None
                        else jnp.where(lanes_at >= m * tile_cols, turned, whole)
                    )
                at = r * tile_rows + q * stripes
                for h in range(local_heads):
                    bias[
                        at : at + stripes,
                        h * total + tile * LANES : h * total + (tile + 1) * LANES,
                    ] = jnp.where(padded, -1e30, whole[h * stripes : (h + 1) * stripes])

    for s in range(samples):
        if n_row > 2:
            pass_on(n_row - 1, s)
        project(s)
        attend(s)
        give(s)

    for k in range(1, n_row):
        if shared:
            for m in range(1, pieces):
                ow_group_wait(k, m)
        else:
            ow_row_wait(k)

    def update_of(source):
        flat = heads_in[source].reshape(samples * token_rows, local_width)
        return jnp.dot(flat, ow[source], preferred_element_type=jnp.float32)

    update = tok[:, me].reshape(samples * token_rows, width).astype(jnp.float32) + 0.0
    product = update_of(me)
    for k in range(1, n_row):
        for s in range(samples):
            att_wait(s, k)
        product = product + update_of(row_peer(n_row - k))
    out[...] = (update + product).astype(out.dtype).reshape(samples, token_rows, width)

    for s in range(samples):
        finish_tok_sends(s)
        for k in range(1, n_row):
            att_copy(s, k).wait_send()
    for k in range(1, n_row):
        bias_row_copy(k).wait_send()
        ow_row_copy(k).wait_send()
        if shared:
            for m in range(1, pieces):
                ow_group_copy(k, m).wait_send()
    for k in range(n_row):
        for m in range(1, n_plane):
            bias_plane_copy(k, m).wait_send()


def per_device(
    axes,
    pair_repr,
    asym_id,
    valid_len,
    rel_embed,
    pair_gain,
    bias_weight,
    tokens,
    token_gain,
    qkv_weight,
    out_weight,
):
    n_job, n_row, n_col, n_samp = axes
    samples, token_rows, width = tokens.shape
    total = n_row * token_rows
    n_plane = n_col * n_samp
    heads = bias_weight.shape[1]
    local_heads = heads // n_row
    tile_rows, tile_cols, channels = pair_repr.shape
    local_width = qkv_weight.shape[-1]
    out_rows = out_weight.shape[1]
    row_pieces = 1 if out_rows % (16 * n_job * n_samp) else n_job * n_samp
    col_pieces = 1 if width % (LANES * n_col) else n_col
    pieces = row_pieces * col_pieces
    stripes = tile_rows // (LANES // tile_cols)
    head_rows = local_heads * stripes
    bf16, f32 = jnp.bfloat16, jnp.float32
    dma = pltpu.SemaphoreType.DMA
    any_spec = pl.BlockSpec(memory_space=pl.ANY)
    return pl.pallas_call(
        functools.partial(kernel, axes, (row_pieces, col_pieces)),
        out_shape=jax.ShapeDtypeStruct(tokens.shape, tokens.dtype),
        in_specs=[any_spec] * 10,
        out_specs=pl.BlockSpec(memory_space=pltpu.VMEM),
        scratch_shapes=[
            pltpu.SMEM(asym_id.shape, jnp.int32),
            pltpu.SMEM(valid_len.shape, jnp.int32),
            pltpu.VMEM(pair_repr.shape, bf16),
            pltpu.VMEM(rel_embed.shape, bf16),
            pltpu.VMEM((1, channels), f32),
            pltpu.VMEM(bias_weight.shape[::-1], bf16),
            pltpu.VMEM(token_gain.shape, f32),
            pltpu.VMEM((3, local_width, width), bf16),
            pltpu.VMEM((samples, n_row, token_rows, width), bf16),
            pltpu.VMEM((n_row, out_rows, width), bf16),
            pltpu.VMEM((heads * stripes, LANES), f32),
            pltpu.VMEM((n_row, n_plane, head_rows, LANES), f32),
            pltpu.VMEM((total, local_heads * total), f32),
            pltpu.VMEM((samples, total, local_width), bf16),
            pltpu.VMEM((samples, total, local_width), bf16),
            pltpu.VMEM((samples, total, local_width), bf16),
            pltpu.VMEM((samples, n_row, token_rows, local_width), bf16),
            pltpu.VMEM((n_row, samples, token_rows, local_width), bf16),
            dma((9,)),
            dma((samples,)),
            dma((2, samples, n_row)),
            dma((samples, n_row)),
            dma((n_row,)),
            dma((n_row,)),
            dma((n_row, n_plane)),
            dma((n_row, n_plane)),
            dma,
            dma((n_row,)),
            dma((n_row,)),
            dma((n_row, pieces)),
            dma((n_row, pieces)),
            dma((samples, n_row)),
            dma((samples, n_row)),
        ],
        compiler_params=pltpu.CompilerParams(
            collective_id=0, has_side_effects=True, vmem_limit_bytes=60 * 1024 * 1024
        ),
    )(
        asym_id,
        valid_len,
        pair_repr,
        rel_embed,
        pair_gain.reshape(1, channels),
        bias_weight.T,
        tokens,
        token_gain,
        jnp.swapaxes(qkv_weight, 2, 3),
        out_weight,
    )


def solution(mesh):
    axes = tuple(mesh.shape[name] for name in ("job", "row", "col", "samp"))
    return jax.shard_map(
        functools.partial(per_device, axes),
        mesh=mesh,
        in_specs=(
            P(("job", "row"), ("col", "samp"), None),
            P("job"),
            P("job"),
            P(),
            P(),
            P(),
            P(("job", "col", "samp"), "row", None),
            P(),
            P(None, None, None, "row"),
            P(None, "row", None),
        ),
        out_specs=P(("job", "col", "samp"), "row", None),
        check_vma=False,
    )
```
